32 devices in a mesh: slab: 4 (over x, core), rep: 8 (over z, y).
Axes of the slice: x: 2, y: 2, z: 4, core: 2. Of those that a mesh axis runs over, the one named last changes fastest.
Arguments:
- image: float32 [144, 256, 256], P('slab', 'rep'), may hold values from 0.5 to 2
- sensitivity: float32 [144, 256, 256], P('slab', 'rep'), may hold values from 0.5 to 2
- system_blocks: bfloat16 [512, 128, 1024], P(('slab', 'rep')), may hold values from 0 to 0.00390625
- tile_slab: int32 [512, 1], P(('slab', 'rep')), may hold values from 0 to 3; in each aligned block of 16 rows (0 to 15, 16 to 31, ...) at most 6 rows name the same one
- tile_block: int32 [512], P(('slab', 'rep')), may hold values from 0 to 2303
- background: bfloat16 [512, 128], P(('slab', 'rep')), may hold values from 0.19921875 to 1
Outputs:
- updated: float32 [144, 256, 256], P('slab', 'rep')
The draws below stay inside these ranges and needn't reach their ends.
Inputs may be any that keep to these rules, and one draw needn't show every extreme that they name: `tile_slab`: among the 16 tiles of one device at most 6 view the same slab, and in some devices some slab is viewed by exactly 6.
All inputs are finite; a program needn't handle non-finite values.
Results may differ from the reference program's by a relative error of at most 0.0003.
Values may be sent and summed in bfloat16 or wider, within the bound.
No kernel may reach another device: no remote copies, remote signals or barrier semaphores. Data moves between devices by JAX's collectives and lax.ppermute only.
A program may use at most 64 MiB of HBM per device.

```python
import math
import jax
import jax.numpy as jnp
import numpy as np
from jax import lax

NX = 256
NY = 256
TILE = 128
VB = 1024
PIECES_PER_CARD = 16
CAP = 6
NZ = 144
NBLK = 2304
TILES = 512
N_SLAB = 4


def place_ends(entries, own_key, smallest, largest):
    dims = entries.shape
    place = [jax.random.randint(jax.random.fold_in(own_key, axis), (), 0, dims[axis]) for axis in range(len(dims))]
    entries = entries.at[tuple(place)].set(smallest)
    longest = dims.index(max(dims))
    place[longest] = (place[longest] + 1) % dims[longest]
    return entries.at[tuple(place)].set(largest)


def level_of(rng, dims, pieces, low, top_value):
    def one(axis_at, blocks):
        draws = jax.random.uniform(jax.random.fold_in(jax.random.fold_in(rng, 6), axis_at), (blocks,), jnp.float32, low / len(pieces), top_value / len(pieces))
        return jnp.repeat(jnp.exp(draws), dims[axis_at] // blocks).reshape((-1,) + (1,) * (len(dims) - axis_at - 1))

    level = one(*pieces[0])
    for cut in pieces[1:]:
        level = level * one(*cut)
    return level


def assign_block(key, own, number, rows, amount, top, limit, skew):
    ranking = jax.random.permutation(key, amount)
    heavy_load, ordinary = portions_of(amount, rows * top, limit, skew, True), portions_of(amount, rows * top, limit, skew, False)
    places = jnp.arange(amount)

    def named(sizes, turn):
        used = int((sizes > 0).sum())
        fixed = max(1, used // 4)
        shifted = fixed + (places - fixed + turn * (used - fixed)) % max(1, amount - fixed)
        return jnp.zeros((amount,), jnp.int32).at[ranking[jnp.where(places < fixed, places, shifted)]].set(jnp.asarray(sizes, jnp.int32))

    sizes = jnp.where(number % 4 == 0, named(heavy_load, number // 4), named(ordinary, number - number // 4 - 1))
    mixed = jax.random.permutation(jax.random.fold_in(own, 3), amount)
    giver, sink = mixed[0:amount // 2 * 2:2], mixed[1:amount // 2 * 2:2]
    margin = jnp.minimum(sizes[giver] - 1, limit - sizes[sink]) // 2
    margin = jnp.where((giver == ranking[0]) | (sink == ranking[0]) | (sizes[sink] == 0), 0, jnp.maximum(margin, 0))
    shifted = jax.random.randint(jax.random.fold_in(own, 4), (amount // 2,), 0, 1 << 20) % (margin + 1)
    sizes = sizes.at[giver].add(-shifted).at[sink].add(shifted)
    labels = jnp.searchsorted(jnp.cumsum(sizes), jnp.arange(rows * top), side="right").astype(jnp.int32)
    listing = labels.reshape(top, rows).T
    listing = listing[jax.random.permutation(jax.random.fold_in(own, 1), rows)]
    turn = jax.random.randint(jax.random.fold_in(own, 2), (rows, 1), 0, top)
    return jnp.take_along_axis(listing, (jnp.arange(top)[None, :] + turn) % top, axis=1)


def portions_of(count, total, reach, skew, full):
    portions = [(1 << 20) // math.isqrt(standing ** skew) + 1 for standing in range(1, count + 1)]
    largest = reach if full else min(reach, max(-(-total // count), total * portions[0] // sum(portions)))
    least = 1 if total - largest >= count - 1 else 0
    given, surplus = [largest] + [least] * (count - 1), total - largest - least * (count - 1)
    while surplus > 0:
        free = [i for i in range(1, count) if given[i] < largest] or [i for i in range(1, count) if given[i] < reach]
        whole, remaining = sum([portions[i] for i in free]), surplus
        for i in free:
            more = min(reach - given[i], max(1, remaining * portions[i] // whole), surplus)
            given[i] = given[i] + more
            surplus = surplus - more
    return np.array(given)


def setup_inputs(seed: int = 0) -> dict:
    splits = jax.random.split(jax.random.key(seed), 7)
    image = jnp.clip(jnp.exp(math.log(2.0) - 1.3862944 * jax.random.uniform(splits[0], (NZ, NY, NX), jnp.float32) ** level_of(splits[0], (NZ, NY, NX), ((0, 4), (1, 8)), -0.2, 0.2)), 0.5, 2.0)
    sensitivity = jnp.clip(jnp.exp(math.log(2.0) - 1.3862944 * jax.random.uniform(splits[1], (NZ, NY, NX), jnp.float32) ** level_of(splits[1], (NZ, NY, NX), ((0, 4), (1, 8)), -0.2, 0.2)), 0.5, 2.0)
    system_blocks = jnp.clip(0.00390625 * jax.random.uniform(splits[2], (TILES, TILE, VB), jnp.float32) ** level_of(splits[2], (TILES, TILE, VB), ((0, 32),), -0.2, 0.2), 0.0, 0.00390625).astype(jnp.bfloat16)
    tile_slab_keys = jax.random.split(jax.random.fold_in(splits[3], 1), TILES // PIECES_PER_CARD)
    tile_slab_turns = jax.random.permutation(jax.random.fold_in(splits[3], 3), TILES // PIECES_PER_CARD)
    tile_slab = jax.vmap(lambda own, number: assign_block(jax.random.fold_in(splits[3], 2), own, number, PIECES_PER_CARD, N_SLAB, 1, CAP, 2))(tile_slab_keys, tile_slab_turns).reshape((TILES, 1))
    tile_block = place_ends(jax.random.randint(splits[4], (TILES,), 0, NBLK), jax.random.fold_in(splits[4], 1), 0, NBLK - 1).astype(jnp.int32)
    background = jnp.clip(jnp.exp(math.log(1.0) - 1.6133518 * jax.random.uniform(splits[5], (TILES, TILE), jnp.float32) ** level_of(splits[5], (TILES, TILE), ((0, 32),), -0.2, 0.2)), 0.19921875, 1.0).astype(jnp.bfloat16)
    return dict(image=image, sensitivity=sensitivity, system_blocks=system_blocks, tile_slab=tile_slab, tile_block=tile_block, background=background)


def reference(image, sensitivity, system_blocks, tile_slab, tile_block, background):
    tile_rows = system_blocks.shape[1]
    width = system_blocks.shape[2]
    unrolled_emission_map = image.astype(jnp.bfloat16).reshape(-1, width)
    index = (tile_slab[:, 0].astype(jnp.int32) * NBLK + tile_block.astype(jnp.int32)).astype(jnp.int32)

    def one_group(group):
        response_operator_lines, rows_index, back_ground = group
        emission_cell_entries = unrolled_emission_map[rows_index].astype(jnp.float32)
        sys_wide = response_operator_lines.astype(jnp.float32)
        forward_projection = jnp.einsum('tev,tv->te', sys_wide, emission_cell_entries, precision=lax.Precision.HIGHEST)
        inverse_permutation = (1.0 / (forward_projection + back_ground.astype(jnp.float32))).astype(jnp.bfloat16)
        inverse_permutation = lax.optimization_barrier(inverse_permutation)
        return jnp.einsum('tev,te->tv', sys_wide, inverse_permutation.astype(jnp.float32), precision=lax.Precision.HIGHEST)

    groups = (system_blocks.reshape(-1, 16, tile_rows, width), index.reshape(-1, 16), background.reshape(-1, 16, tile_rows))
    backproj = lax.map(one_group, groups).reshape(-1, width)
    partial_value = jnp.zeros(unrolled_emission_map.shape, jnp.float32).at[index].add(backproj)
    return image * partial_value.reshape(image.shape) / sensitivity
```

```python
import functools
import jax
import jax.numpy as jnp
from jax import lax
from jax.experimental import pallas as pl
from jax.experimental.pallas import tpu as pltpu
from jax.sharding import PartitionSpec as P

CAP = 6
LANES = 128
SUB = 8
AXES = ("slab", "rep")
SMEM = pltpu.SMEM
VMEM = pltpu.VMEM


def spec(space):
    return pl.BlockSpec(memory_space=space)


def half_rows():
    return lax.broadcasted_iota(jnp.int32, (SUB, LANES), 0) < SUB // 2


def route_kernel(slab_ref, block_ref, ids_ref, slot_ref, *, peers, reps, per_plane, per_owner, cap):
    for d in range(peers):
        ids_ref[d * LANES] = 0
    for t in range(slot_ref.shape[0]):
        block = block_ref[t]
        plane = lax.div(block, per_plane)
        within = lax.rem(block, per_plane)
        d = slab_ref[t] * reps + lax.div(within, per_owner)
        position = ids_ref[d * LANES]
        ids_ref[d * LANES] = position + 1
        ids_ref[d * LANES + 1 + position] = plane * per_owner + lax.rem(within, per_owner)
        slot_ref[t] = d * cap + position


def serve_kernel(ids_ref, image_ref, out_ref, *, peers, cap):
    top = half_rows()

    def peer(d, carry):
        def row(j, inner):
            local_id = ids_ref[d * LANES + 1 + j]
            tile = image_ref[lax.div(local_id, 2)]
            left, right = tile[:, :LANES], tile[:, LANES:]
            even = jnp.where(top, left, pltpu.roll(right, SUB // 2, 0))
            odd = jnp.where(top, pltpu.roll(left, SUB // 2, 0), right)
            picked = jnp.where(lax.rem(local_id, 2) == 0, even, odd)
            out_ref[d * cap + j] = picked.astype(jnp.bfloat16)
            return inner

        return lax.fori_loop(0, ids_ref[d * LANES], row, carry)

    lax.fori_loop(0, peers, peer, 0)


def project_kernel(slot_ref, blocks_ref, system_ref, background_ref, out_ref):
    half = SUB // 2
    order = [(k % 2) * half + k // 2 for k in range(SUB)]
    for t in range(system_ref.shape[0]):
        slot = slot_ref[t]
        block = blocks_ref[slot].astype(jnp.float32)
        line = jnp.concatenate([block[j : j + 1] for j in order], axis=1).astype(jnp.bfloat16)
        system = system_ref[t]
        forward = lax.dot_general(
            line, system, (((1,), (1,)), ((), ())), preferred_element_type=jnp.float32
        )
        inverse = (1.0 / (forward + background_ref[t : t + 1].astype(jnp.float32))).astype(
            jnp.bfloat16
        )
        back = jnp.dot(inverse, system, preferred_element_type=jnp.float32)
        out_ref[slot] = jnp.concatenate(
            [back[:, order.index(j) * LANES : (order.index(j) + 1) * LANES] for j in range(SUB)],
            axis=0,
        )


def update_kernel(ids_ref, back_ref, image_ref, sensitivity_ref, out_ref, *, peers, cap):
    top = half_rows()
    out_ref[...] = jnp.zeros(out_ref.shape, jnp.float32)

    def peer(d, carry):
        def row(j, inner):
            local_id = ids_ref[d * LANES + 1 + j]
            group = lax.div(local_id, 2)
            even = lax.rem(local_id, 2) == 0
            block = back_ref[d * cap + j]
            turned = pltpu.roll(block, SUB // 2, 0)
            left = jnp.where(even, jnp.where(top, block, 0.0), jnp.where(top, 0.0, turned))
            right = jnp.where(even, jnp.where(top, turned, 0.0), jnp.where(top, 0.0, block))
            out_ref[group] = out_ref[group] + jnp.concatenate([left, right], axis=1)
            return inner

        return lax.fori_loop(0, ids_ref[d * LANES], row, carry)

    lax.fori_loop(0, peers, peer, 0)
    out_ref[...] = image_ref[...] * out_ref[...] / sensitivity_ref[...]


def local(image, sensitivity, system_blocks, tile_slab, tile_block, background):
    reps = lax.axis_size("rep")
    peers = lax.axis_size("slab") * reps
    tiles_here, _, width = system_blocks.shape
    planes, local_rows, columns = image.shape
    assert columns == 2 * LANES and width == SUB * LANES and local_rows % SUB == 0
    per_owner = local_rows * columns // width
    cap = CAP
    ids, slot = pl.pallas_call(
        functools.partial(
            route_kernel,
            peers=peers,
            reps=reps,
            per_plane=per_owner * reps,
            per_owner=per_owner,
            cap=cap,
        ),
        in_specs=[spec(SMEM), spec(SMEM)],
        out_specs=(spec(SMEM), spec(SMEM)),
        out_shape=(
            jax.ShapeDtypeStruct((peers * LANES,), jnp.int32),
            jax.ShapeDtypeStruct((tiles_here,), jnp.int32),
        ),
        name="route",
    )(tile_slab.reshape(-1), tile_block)

    def exchange(array):
        return lax.all_to_all(array, AXES, split_axis=0, concat_axis=0, tiled=True)

    asked = exchange(ids.reshape(peers, LANES)).reshape(-1)
    image_tiles = image.reshape(-1, SUB, columns)
    served = pl.pallas_call(
        functools.partial(serve_kernel, peers=peers, cap=cap),
        in_specs=[spec(SMEM), spec(VMEM)],
        out_specs=spec(VMEM),
        out_shape=jax.ShapeDtypeStruct((peers * cap, SUB, LANES), jnp.bfloat16),
        name="serve",
    )(asked, image_tiles)
    blocks = exchange(served.reshape(peers, cap, SUB, LANES)).reshape(served.shape)
    back = pl.pallas_call(
        project_kernel,
        in_specs=[spec(SMEM), spec(VMEM), spec(VMEM), spec(VMEM)],
        out_specs=spec(VMEM),
        out_shape=jax.ShapeDtypeStruct(served.shape, jnp.float32),
        name="project",
    )(slot, blocks, system_blocks, background)
    received = exchange(back.reshape(peers, cap, SUB, LANES)).reshape(back.shape)
    updated = pl.pallas_call(
        functools.partial(update_kernel, peers=peers, cap=cap),
        in_specs=[spec(SMEM), spec(VMEM), spec(VMEM), spec(VMEM)],
        out_specs=spec(VMEM),
        out_shape=jax.ShapeDtypeStruct(image_tiles.shape, jnp.float32),
        name="update",
    )(asked, received, image_tiles, sensitivity.reshape(image_tiles.shape))
    return updated.reshape(image.shape)


def solution(mesh):
    return jax.shard_map(
        local,
        mesh=mesh,
        in_specs=(
            P("slab", "rep", None),
            P("slab", "rep", None),
            P(("slab", "rep"), None, None),
            P(("slab", "rep"), None),
            P(("slab", "rep")),
            P(("slab", "rep"), None),
        ),
        out_specs=P("slab", "rep", None),
        check_vma=False,
    )
```

```python
import functools
import jax
import jax.numpy as jnp
from jax import lax
from jax.experimental import pallas as pl
from jax.experimental.pallas import tpu as pltpu
from jax.sharding import PartitionSpec as P

CAP = 6
LANES = 128
SUB = 8
AXES = ("slab", "rep")
SMEM = pltpu.SMEM
VMEM = pltpu.VMEM
PARAMS = pltpu.CompilerParams(vmem_limit_bytes=8 << 20)
CODE_TOP = 32000.0
LEAST = 2.0**-100


def spec(space):
    return pl.BlockSpec(memory_space=space)


def half_rows():
    return lax.broadcasted_iota(jnp.int32, (SUB, LANES), 0) < SUB // 2


def route_kernel(slab_ref, block_ref, ids_ref, slot_ref, *, peers, reps, per_plane, per_owner):
    for d in range(peers):
        ids_ref[d * LANES] = 0
    for t in range(slot_ref.shape[0]):
        block = block_ref[t]
        plane = lax.div(block, per_plane)
        within = lax.rem(block, per_plane)
        d = slab_ref[t] * reps + lax.div(within, per_owner)
        position = ids_ref[d * LANES]
        ids_ref[d * LANES] = position + 1
        ids_ref[d * LANES + 1 + position] = plane * per_owner + lax.rem(within, per_owner)
        slot_ref[t] = d * SUB + position


def serve_kernel(ids_ref, image_ref, out_ref, *, peers, cap):
    top = half_rows()

    def peer(d, carry):
        def row(j, inner):
            local_id = ids_ref[d * LANES + 1 + j]
            tile = image_ref[lax.div(local_id, 2)]
            left, right = tile[:, :LANES], tile[:, LANES:]
            even = jnp.where(top, left, pltpu.roll(right, SUB // 2, 0))
            odd = jnp.where(top, pltpu.roll(left, SUB // 2, 0), right)
            picked = jnp.where(lax.rem(local_id, 2) == 0, even, odd)
            out_ref[d * cap + j] = picked.astype(jnp.bfloat16)
            return inner

        return lax.fori_loop(0, ids_ref[d * LANES], row, carry)

    lax.fori_loop(0, peers, peer, 0)


def project_kernel(slot_ref, blocks_ref, system_ref, background_ref, out_ref, power_ref, *, peers, cap):
    half = SUB // 2
    order = [(k % 2) * half + k // 2 for k in range(SUB)]
    for t in range(system_ref.shape[0]):
        d, position = lax.div(slot_ref[t], SUB), lax.rem(slot_ref[t], SUB)
        block = blocks_ref[d * cap + position].astype(jnp.float32)
        line = jnp.concatenate([block[j : j + 1] for j in order], axis=1).astype(jnp.bfloat16)
        system = system_ref[t]
        forward = lax.dot_general(
            line, system, (((1,), (1,)), ((), ())), preferred_element_type=jnp.float32
        )
        inverse = (1.0 / (forward + background_ref[t : t + 1].astype(jnp.float32))).astype(
            jnp.bfloat16
        )
        back = jnp.dot(inverse, system, preferred_element_type=jnp.float32)
        largest = jnp.broadcast_to(jnp.max(back, axis=1, keepdims=True), (1, LANES))
        power = jnp.ceil(jnp.log2(jnp.maximum(largest, LEAST)))
        power_ref[d, pl.ds(position, 1)] = power.astype(jnp.int32)
        tile = jnp.concatenate(
            [back[:, order.index(j) * LANES : (order.index(j) + 1) * LANES] for j in range(SUB)],
            axis=0,
        )
        codes = tile * (CODE_TOP * jnp.exp2(-power)) + 0.5
        out_ref[d * (cap + 1) + position] = codes.astype(jnp.int32).astype(jnp.int16)
    for d in range(peers):
        out_ref[d * (cap + 1) + cap] = power_ref[d].astype(jnp.int16)


def update_kernel(ids_ref, back_ref, image_ref, sensitivity_ref, out_ref, *, peers, cap):
    top = half_rows()
    sublane = lax.broadcasted_iota(jnp.int32, (SUB, LANES), 0)
    out_ref[...] = jnp.zeros(out_ref.shape, jnp.float32)

    def peer(d, carry):
        powers = back_ref[d * (cap + 1) + cap].astype(jnp.int32)

        def row(j, inner):
            local_id = ids_ref[d * LANES + 1 + j]
            group = lax.div(local_id, 2)
            even = lax.rem(local_id, 2) == 0
            power = jnp.sum(jnp.where(sublane == j, powers, 0), axis=0, keepdims=True)
            step = jnp.exp2(power.astype(jnp.float32)) * (1.0 / CODE_TOP)
            block = back_ref[d * (cap + 1) + j].astype(jnp.int32).astype(jnp.float32) * step
            turned = pltpu.roll(block, SUB // 2, 0)
            left = jnp.where(even, jnp.where(top, block, 0.0), jnp.where(top, 0.0, turned))
            right = jnp.where(even, jnp.where(top, turned, 0.0), jnp.where(top, 0.0, block))
            out_ref[group] = out_ref[group] + jnp.concatenate([left, right], axis=1)
            return inner

        return lax.fori_loop(0, ids_ref[d * LANES], row, carry)

    lax.fori_loop(0, peers, peer, 0)
    out_ref[...] = image_ref[...] * out_ref[...] / sensitivity_ref[...]


def local(image, sensitivity, system_blocks, tile_slab, tile_block, background):
    reps = lax.axis_size("rep")
    peers = lax.axis_size("slab") * reps
    tiles_here, _, width = system_blocks.shape
    planes, local_rows, columns = image.shape
    assert columns == 2 * LANES and width == SUB * LANES and local_rows % SUB == 0
    per_owner = local_rows * columns // width
    cap = CAP
    ids, slot = pl.pallas_call(
        functools.partial(
            route_kernel,
            peers=peers,
            reps=reps,
            per_plane=per_owner * reps,
            per_owner=per_owner,
        ),
        in_specs=[spec(SMEM), spec(SMEM)],
        out_specs=(spec(SMEM), spec(SMEM)),
        out_shape=(
            jax.ShapeDtypeStruct((peers * LANES,), jnp.int32),
            jax.ShapeDtypeStruct((tiles_here,), jnp.int32),
        ),
        compiler_params=PARAMS,
        name="route",
    )(tile_slab.reshape(-1), tile_block)

    def exchange(array):
        return lax.all_to_all(array, AXES, split_axis=0, concat_axis=0, tiled=True)

    asked = exchange(ids.reshape(peers, LANES)).reshape(-1)
    image_tiles = image.reshape(-1, SUB, columns)
    served = pl.pallas_call(
        functools.partial(serve_kernel, peers=peers, cap=cap),
        in_specs=[spec(SMEM), spec(VMEM)],
        out_specs=spec(VMEM),
        out_shape=jax.ShapeDtypeStruct((peers * cap, SUB, LANES), jnp.bfloat16),
        compiler_params=PARAMS,
        name="serve",
    )(asked, image_tiles)
    blocks = exchange(served.reshape(peers, cap, SUB, LANES)).reshape(served.shape)
    back = pl.pallas_call(
        functools.partial(project_kernel, peers=peers, cap=cap),
        in_specs=[spec(SMEM), spec(VMEM), spec(VMEM), spec(VMEM)],
        out_specs=spec(VMEM),
        out_shape=jax.ShapeDtypeStruct((peers * (cap + 1), SUB, LANES), jnp.int16),
        scratch_shapes=[pltpu.VMEM((peers, SUB, LANES), jnp.int32)],
        compiler_params=PARAMS,
        name="project",
    )(slot, blocks, system_blocks, background)
    received = exchange(back.reshape(peers, cap + 1, SUB, LANES)).reshape(back.shape)
    updated = pl.pallas_call(
        functools.partial(update_kernel, peers=peers, cap=cap),
        in_specs=[spec(SMEM), spec(VMEM), spec(VMEM), spec(VMEM)],
        out_specs=spec(VMEM),
        out_shape=jax.ShapeDtypeStruct(image_tiles.shape, jnp.float32),
        compiler_params=PARAMS,
        name="update",
    )(asked, received, image_tiles, sensitivity.reshape(image_tiles.shape))
    return updated.reshape(image.shape)


def solution(mesh):
    return jax.shard_map(
        local,
        mesh=mesh,
        in_specs=(
            P("slab", "rep", None),
            P("slab", "rep", None),
            P(("slab", "rep"), None, None),
            P(("slab", "rep"), None),
            P(("slab", "rep")),
            P(("slab", "rep"), None),
        ),
        out_specs=P("slab", "rep", None),
        check_vma=False,
    )
```

```python
import functools
import jax
import jax.numpy as jnp
from jax import lax
from jax.experimental import pallas as pl
from jax.experimental.pallas import tpu as pltpu
from jax.sharding import PartitionSpec as P

CAP = 6
LANES = 128
SUB = 8
AXES = ("slab", "rep")
SMEM = pltpu.SMEM
VMEM = pltpu.VMEM
PARAMS = pltpu.CompilerParams(vmem_limit_bytes=8 << 20)
CODE_TOP = 32000.0
LEAST = 2.0**-100
WIDE = pltpu.CompilerParams(vmem_limit_bytes=52 << 20)


def spec(space):
    return pl.BlockSpec(memory_space=space)


def half_rows():
    return lax.broadcasted_iota(jnp.int32, (SUB, LANES), 0) < SUB // 2


def route_kernel(
    slab_in, block_in, ids_ref, slot_ref, slab_ref, block_ref, sems, *, peers, reps, per_plane, per_owner
):
    copies = (
        pltpu.make_async_copy(slab_in, slab_ref, sems.at[0]),
        pltpu.make_async_copy(block_in, block_ref, sems.at[1]),
    )
    for copy in copies:
        copy.start()
    for d in range(peers):
        ids_ref[d * LANES] = 0
    for copy in copies:
        copy.wait()
    for t in range(slot_ref.shape[0]):
        block = block_ref[t]
        plane = lax.div(block, per_plane)
        within = lax.rem(block, per_plane)
        d = slab_ref[t] * reps + lax.div(within, per_owner)
        position = ids_ref[d * LANES]
        ids_ref[d * LANES] = position + 1
        ids_ref[d * LANES + 1 + position] = plane * per_owner + lax.rem(within, per_owner)
        slot_ref[t] = d * SUB + position


def serve_kernel(ids_ref, image_ref, out_ref, list_ref, *, peers, cap):
    top = half_rows()

    def peer(d, carry):
        def row(j, inner):
            local_id = ids_ref[d * LANES + 1 + j]
            list_ref[1 + 2 * inner] = d * SUB + j
            list_ref[2 + 2 * inner] = local_id
            tile = image_ref[lax.div(local_id, 2)]
            left, right = tile[:, :LANES], tile[:, LANES:]
            even = jnp.where(top, left, pltpu.roll(right, SUB // 2, 0))
            odd = jnp.where(top, pltpu.roll(left, SUB // 2, 0), right)
            picked = jnp.where(lax.rem(local_id, 2) == 0, even, odd)
            out_ref[d * cap + j] = picked.astype(jnp.bfloat16)
            return inner + 1

        return lax.fori_loop(0, ids_ref[d * LANES], row, carry)

    list_ref[0] = lax.fori_loop(0, peers, peer, 0)


def project_kernel(
    slot_ref, blocks_ref, system_in, background_ref, out_ref, line_ref, power_ref, system_ref, sems,
    *, peers, cap
):
    half = SUB // 2
    tiles, tile_rows, width = system_ref.shape
    copies = [
        pltpu.make_async_copy(system_in.at[t], system_ref.at[t], sems.at[t]) for t in range(tiles)
    ]
    for copy in copies:
        copy.start()
    order = [(k % 2) * half + k // 2 for k in range(SUB)]
    places = [(lax.div(slot_ref[t], SUB), lax.rem(slot_ref[t], SUB)) for t in range(tiles)]
    for t, (d, position) in enumerate(places):
        block = blocks_ref[d * cap + position].astype(jnp.float32)
        for k, j in enumerate(order):
            line_ref[t : t + 1, k * LANES : (k + 1) * LANES] = block[j : j + 1]
    lines = line_ref[...].astype(jnp.bfloat16)
    row = lax.broadcasted_iota(jnp.int32, (tiles, tile_rows), 0)
    forward = jnp.zeros((tiles, tile_rows), jnp.float32)
    for t in range(tiles):
        copies[t].wait()
        every = lax.dot_general(
            lines, system_ref[t], (((1,), (1,)), ((), ())), preferred_element_type=jnp.float32
        )
        forward = jnp.where(row == t, every, forward)
    inverse = (1.0 / (forward + background_ref[...].astype(jnp.float32))).astype(jnp.bfloat16)
    for t in range(tiles):
        every = jnp.dot(inverse, system_ref[t], preferred_element_type=jnp.float32)
        line_ref[t : t + 1, :] = every[t : t + 1, :]
    back = line_ref[...]
    largest = jnp.broadcast_to(jnp.max(back, axis=1, keepdims=True), (tiles, LANES))
    power = jnp.ceil(jnp.log2(jnp.maximum(largest, LEAST)))
    scale = CODE_TOP * jnp.exp2(-power)
    power = power.astype(jnp.int32)
    codes = [
        (back[:, k * LANES : (k + 1) * LANES] * scale + 0.5).astype(jnp.int32) for k in range(SUB)
    ]
    for t, (d, position) in enumerate(places):
        power_ref[d, pl.ds(position, 1)] = power[t : t + 1]
        tile = jnp.concatenate([codes[order.index(j)][t : t + 1] for j in range(SUB)], axis=0)
        out_ref[d * (cap + 1) + position] = tile.astype(jnp.int16)
    for d in range(peers):
        out_ref[d * (cap + 1) + cap] = power_ref[d].astype(jnp.int16)


def update_kernel(
    list_ref, back_ref, image_ref, sensitivity_ref, out_ref, step_ref, *, peers, cap
):
    top = half_rows()
    out_ref[...] = jnp.zeros(out_ref.shape, jnp.float32)
    for d in range(peers):
        powers = back_ref[d * (cap + 1) + cap].astype(jnp.int32).astype(jnp.float32)
        step_ref[d] = jnp.exp2(powers) * (1.0 / CODE_TOP)

    def request(i, carry):
        place = list_ref[1 + 2 * i]
        local_id = list_ref[2 + 2 * i]
        d, j = lax.div(place, SUB), lax.rem(place, SUB)
        group = lax.div(local_id, 2)
        even = lax.rem(local_id, 2) == 0
        step = step_ref[d, pl.ds(j, 1)]
        block = back_ref[d * (cap + 1) + j].astype(jnp.int32).astype(jnp.float32) * step
        turned = pltpu.roll(block, SUB // 2, 0)
        left = jnp.where(even, jnp.where(top, block, 0.0), jnp.where(top, 0.0, turned))
        right = jnp.where(even, jnp.where(top, turned, 0.0), jnp.where(top, 0.0, block))
        out_ref[group] = out_ref[group] + jnp.concatenate([left, right], axis=1)
        return carry

    lax.fori_loop(0, list_ref[0], request, 0)
    out_ref[...] = image_ref[...] * out_ref[...] / sensitivity_ref[...]


def local(image, sensitivity, system_blocks, tile_slab, tile_block, background):
    reps = lax.axis_size("rep")
    peers = lax.axis_size("slab") * reps
    tiles_here, _, width = system_blocks.shape
    planes, local_rows, columns = image.shape
    assert columns == 2 * LANES and width == SUB * LANES and local_rows % SUB == 0
    per_owner = local_rows * columns // width
    cap = CAP
    ids, slot = pl.pallas_call(
        functools.partial(
            route_kernel,
            peers=peers,
            reps=reps,
            per_plane=per_owner * reps,
            per_owner=per_owner,
        ),
        in_specs=[spec(pltpu.HBM), spec(pltpu.HBM)],
        out_specs=(spec(SMEM), spec(SMEM)),
        scratch_shapes=[
            pltpu.SMEM((tiles_here,), jnp.int32),
            pltpu.SMEM((tiles_here,), jnp.int32),
            pltpu.SemaphoreType.DMA((2,)),
        ],
        out_shape=(
            jax.ShapeDtypeStruct((peers * LANES,), jnp.int32),
            jax.ShapeDtypeStruct((tiles_here,), jnp.int32),
        ),
        name="route",
    )(tile_slab.reshape(-1), tile_block)

    def exchange(array):
        return lax.all_to_all(array, AXES, split_axis=0, concat_axis=0, tiled=True)

    asked = exchange(ids.reshape(peers, LANES)).reshape(-1)
    image_tiles = image.reshape(-1, SUB, columns)
    served, requests = pl.pallas_call(
        functools.partial(serve_kernel, peers=peers, cap=cap),
        in_specs=[spec(SMEM), spec(VMEM)],
        out_specs=(spec(VMEM), spec(SMEM)),
        out_shape=(
            jax.ShapeDtypeStruct((peers * cap, SUB, LANES), jnp.bfloat16),
            jax.ShapeDtypeStruct((1 + 2 * peers * cap,), jnp.int32),
        ),
        compiler_params=PARAMS,
        name="serve",
    )(asked, image_tiles)
    blocks = exchange(served.reshape(peers, cap, SUB, LANES)).reshape(served.shape)
    back = pl.pallas_call(
        functools.partial(project_kernel, peers=peers, cap=cap),
        in_specs=[spec(SMEM), spec(VMEM), spec(pltpu.HBM), spec(VMEM)],
        out_specs=spec(VMEM),
        out_shape=jax.ShapeDtypeStruct((peers * (cap + 1), SUB, LANES), jnp.int16),
        scratch_shapes=[
            pltpu.VMEM((tiles_here, width), jnp.float32),
            pltpu.VMEM((peers, SUB, LANES), jnp.int32),
            pltpu.VMEM(system_blocks.shape, jnp.bfloat16),
            pltpu.SemaphoreType.DMA((tiles_here,)),
        ],
        compiler_params=WIDE,
        name="project",
    )(slot, blocks, system_blocks, background)
    received = exchange(back.reshape(peers, cap + 1, SUB, LANES)).reshape(back.shape)
    updated = pl.pallas_call(
        functools.partial(update_kernel, peers=peers, cap=cap),
        in_specs=[spec(SMEM), spec(VMEM), spec(VMEM), spec(VMEM)],
        out_specs=spec(VMEM),
        out_shape=jax.ShapeDtypeStruct(image_tiles.shape, jnp.float32),
        scratch_shapes=[pltpu.VMEM((peers, SUB, LANES), jnp.float32)],
        compiler_params=PARAMS,
        name="update",
    )(requests, received, image_tiles, sensitivity.reshape(image_tiles.shape))
    return updated.reshape(image.shape)


def solution(mesh):
    return jax.shard_map(
        local,
        mesh=mesh,
        in_specs=(
            P("slab", "rep", None),
            P("slab", "rep", None),
            P(("slab", "rep"), None, None),
            P(("slab", "rep"), None),
            P(("slab", "rep")),
            P(("slab", "rep"), None),
        ),
        out_specs=P("slab", "rep", None),
        check_vma=False,
    )
```

```python
import functools
import jax
import jax.numpy as jnp
from jax import lax
from jax.experimental import pallas as pl
from jax.experimental.pallas import tpu as pltpu
from jax.sharding import PartitionSpec as P

CAP = 6
LANES = 128
SUB = 8
AXES = ("slab", "rep")
SMEM = pltpu.SMEM
VMEM = pltpu.VMEM
PARAMS = pltpu.CompilerParams(vmem_limit_bytes=8 << 20)
CODE_TOP = 32000.0
LEAST = 2.0**-100
WIDE = pltpu.CompilerParams(vmem_limit_bytes=52 << 20)


def spec(space):
    return pl.BlockSpec(memory_space=space)


def half_rows():
    return lax.broadcasted_iota(jnp.int32, (SUB, LANES), 0) < SUB // 2


def route_kernel(
    slab_in, block_in, ids_ref, slot_ref, slab_ref, block_ref, sems, *, peers, reps, per_plane, per_owner
):
    copies = (
        pltpu.make_async_copy(slab_in, slab_ref, sems.at[0]),
        pltpu.make_async_copy(block_in, block_ref, sems.at[1]),
    )
    for copy in copies:
        copy.start()
    for d in range(peers):
        ids_ref[d * LANES] = 0
    for copy in copies:
        copy.wait()
    for t in range(slot_ref.shape[0]):
        block = block_ref[t]
        plane = lax.div(block, per_plane)
        within = lax.rem(block, per_plane)
        d = slab_ref[t] * reps + lax.div(within, per_owner)
        position = ids_ref[d * LANES]
        ids_ref[d * LANES] = position + 1
        ids_ref[d * LANES + 1 + position] = plane * per_owner + lax.rem(within, per_owner)
        slot_ref[t] = d * SUB + position


def serve_kernel(ids_ref, image_ref, out_ref, list_ref, *, peers, cap):
    top = half_rows()

    def peer(d, carry):
        def row(j, inner):
            local_id = ids_ref[d * LANES + 1 + j]
            list_ref[1 + 2 * inner] = d * SUB + j
            list_ref[2 + 2 * inner] = local_id
            tile = image_ref[lax.div(local_id, 2)]
            left, right = tile[:, :LANES], tile[:, LANES:]
            even = jnp.where(top, left, pltpu.roll(right, SUB // 2, 0))
            odd = jnp.where(top, pltpu.roll(left, SUB // 2, 0), right)
            picked = jnp.where(lax.rem(local_id, 2) == 0, even, odd)
            out_ref[d * cap + j] = picked.astype(jnp.bfloat16)
            return inner + 1

        return lax.fori_loop(0, ids_ref[d * LANES], row, carry)

    list_ref[0] = lax.fori_loop(0, peers, peer, 0)


def project_kernel(
    slot_ref, blocks_ref, system_in, background_ref, out_ref, line_ref, power_ref, system_ref, sems,
    *, peers, cap
):
    half = SUB // 2
    tiles, tile_rows, width = system_ref.shape
    copies = [
        pltpu.make_async_copy(system_in.at[t], system_ref.at[t], sems.at[t]) for t in range(tiles)
    ]
    for copy in copies:
        copy.start()
    order = [(k % 2) * half + k // 2 for k in range(SUB)]
    places = [(lax.div(slot_ref[t], SUB), lax.rem(slot_ref[t], SUB)) for t in range(tiles)]
    for t, (d, position) in enumerate(places):
        block = blocks_ref[d * cap + position].astype(jnp.float32)
        for k, j in enumerate(order):
            line_ref[t : t + 1, k * LANES : (k + 1) * LANES] = block[j : j + 1]
    lines = line_ref[...].T.astype(jnp.bfloat16)
    column = lax.broadcasted_iota(jnp.int32, (tile_rows, tiles), 1)
    forward = jnp.zeros((tile_rows, tiles), jnp.float32)
    for t in range(tiles):
        copies[t].wait()
        every = jnp.dot(system_ref[t], lines, preferred_element_type=jnp.float32)
        forward = jnp.where(column == t, every, forward)
    inverse = (1.0 / (forward.T + background_ref[...].astype(jnp.float32))).astype(jnp.bfloat16)
    for t in range(tiles):
        every = jnp.dot(inverse, system_ref[t], preferred_element_type=jnp.float32)
        line_ref[t : t + 1, :] = every[t : t + 1, :]
    back = line_ref[...]
    largest = jnp.broadcast_to(jnp.max(back, axis=1, keepdims=True), (tiles, LANES))
    power = jnp.ceil(jnp.log2(jnp.maximum(largest, LEAST)))
    scale = CODE_TOP * jnp.exp2(-power)
    power = power.astype(jnp.int32)
    codes = [
        (back[:, k * LANES : (k + 1) * LANES] * scale + 0.5).astype(jnp.int32) for k in range(SUB)
    ]
    for t, (d, position) in enumerate(places):
        power_ref[d, pl.ds(position, 1)] = power[t : t + 1]
        tile = jnp.concatenate([codes[order.index(j)][t : t + 1] for j in range(SUB)], axis=0)
        out_ref[d * (cap + 1) + position] = tile.astype(jnp.int16)
    for d in range(peers):
        out_ref[d * (cap + 1) + cap] = power_ref[d].astype(jnp.int16)


def update_kernel(
    list_ref, back_ref, image_ref, sensitivity_ref, out_ref, step_ref, *, peers, cap
):
    top = half_rows()
    out_ref[...] = jnp.zeros(out_ref.shape, jnp.float32)
    for d in range(peers):
        powers = back_ref[d * (cap + 1) + cap].astype(jnp.int32).astype(jnp.float32)
        step_ref[d] = jnp.exp2(powers) * (1.0 / CODE_TOP)

    def request(i, carry):
        place = list_ref[1 + 2 * i]
        local_id = list_ref[2 + 2 * i]
        d, j = lax.div(place, SUB), lax.rem(place, SUB)
        group = lax.div(local_id, 2)
        even = lax.rem(local_id, 2) == 0
        step = step_ref[d, pl.ds(j, 1)]
        block = back_ref[d * (cap + 1) + j].astype(jnp.int32).astype(jnp.float32) * step
        turned = pltpu.roll(block, SUB // 2, 0)
        left = jnp.where(even, jnp.where(top, block, 0.0), jnp.where(top, 0.0, turned))
        right = jnp.where(even, jnp.where(top, turned, 0.0), jnp.where(top, 0.0, block))
        out_ref[group] = out_ref[group] + jnp.concatenate([left, right], axis=1)
        return carry

    lax.fori_loop(0, list_ref[0], request, 0)
    out_ref[...] = image_ref[...] * out_ref[...] / sensitivity_ref[...]


def local(image, sensitivity, system_blocks, tile_slab, tile_block, background):
    reps = lax.axis_size("rep")
    peers = lax.axis_size("slab") * reps
    tiles_here, _, width = system_blocks.shape
    planes, local_rows, columns = image.shape
    assert columns == 2 * LANES and width == SUB * LANES and local_rows % SUB == 0
    per_owner = local_rows * columns // width
    cap = CAP
    ids, slot = pl.pallas_call(
        functools.partial(
            route_kernel,
            peers=peers,
            reps=reps,
            per_plane=per_owner * reps,
            per_owner=per_owner,
        ),
        in_specs=[spec(pltpu.HBM), spec(pltpu.HBM)],
        out_specs=(spec(SMEM), spec(SMEM)),
        scratch_shapes=[
            pltpu.SMEM((tiles_here,), jnp.int32),
            pltpu.SMEM((tiles_here,), jnp.int32),
            pltpu.SemaphoreType.DMA((2,)),
        ],
        out_shape=(
            jax.ShapeDtypeStruct((peers * LANES,), jnp.int32),
            jax.ShapeDtypeStruct((tiles_here,), jnp.int32),
        ),
        name="route",
    )(tile_slab.reshape(-1), tile_block)

    def exchange(array):
        return lax.all_to_all(array, AXES, split_axis=0, concat_axis=0, tiled=True)

    asked = exchange(ids.reshape(peers, LANES)).reshape(-1)
    image_tiles = image.reshape(-1, SUB, columns)
    served, requests = pl.pallas_call(
        functools.partial(serve_kernel, peers=peers, cap=cap),
        in_specs=[spec(SMEM), spec(VMEM)],
        out_specs=(spec(VMEM), spec(SMEM)),
        out_shape=(
            jax.ShapeDtypeStruct((peers * cap, SUB, LANES), jnp.bfloat16),
            jax.ShapeDtypeStruct((1 + 2 * peers * cap,), jnp.int32),
        ),
        compiler_params=PARAMS,
        name="serve",
    )(asked, image_tiles)
    blocks = exchange(served.reshape(peers, cap, SUB, LANES)).reshape(served.shape)
    back = pl.pallas_call(
        functools.partial(project_kernel, peers=peers, cap=cap),
        in_specs=[spec(SMEM), spec(VMEM), spec(pltpu.HBM), spec(VMEM)],
        out_specs=spec(VMEM),
        out_shape=jax.ShapeDtypeStruct((peers * (cap + 1), SUB, LANES), jnp.int16),
        scratch_shapes=[
            pltpu.VMEM((tiles_here, width), jnp.float32),
            pltpu.VMEM((peers, SUB, LANES), jnp.int32),
            pltpu.VMEM(system_blocks.shape, jnp.bfloat16),
            pltpu.SemaphoreType.DMA((tiles_here,)),
        ],
        compiler_params=WIDE,
        name="project",
    )(slot, blocks, system_blocks, background)
    received = exchange(back.reshape(peers, cap + 1, SUB, LANES)).reshape(back.shape)
    updated = pl.pallas_call(
        functools.partial(update_kernel, peers=peers, cap=cap),
        in_specs=[spec(SMEM), spec(VMEM), spec(VMEM), spec(VMEM)],
        out_specs=spec(VMEM),
        out_shape=jax.ShapeDtypeStruct(image_tiles.shape, jnp.float32),
        scratch_shapes=[pltpu.VMEM((peers, SUB, LANES), jnp.float32)],
        compiler_params=PARAMS,
        name="update",
    )(requests, received, image_tiles, sensitivity.reshape(image_tiles.shape))
    return updated.reshape(image.shape)


def solution(mesh):
    return jax.shard_map(
        local,
        mesh=mesh,
        in_specs=(
            P("slab", "rep", None),
            P("slab", "rep", None),
            P(("slab", "rep"), None, None),
            P(("slab", "rep"), None),
            P(("slab", "rep")),
            P(("slab", "rep"), None),
        ),
        out_specs=P("slab", "rep", None),
        check_vma=False,
    )
```
